32 devices in a mesh: row: 4 (over x, core), col: 8 (over z, y).
Axes of the slice: x: 2, y: 2, z: 4, core: 2. Of those that a mesh axis runs over, the one named last changes fastest.
Arguments:
- w_rec: bfloat16 [2, 4096, 4, 4096], P(None, 'row', None, 'col'), may hold values from -0.09375 to 0.09375
- w_in: bfloat16 [2, 4096, 4, 4096], P(None, 'row', None, 'col'), may hold values from -0.09375 to 0.09375
- gate_pre: float32 [2, 6, 64, 4, 4096], P(None, None, None, None, 'col'), may hold values from -8 to 8, as said below
- cells: float32 [2, 7, 64, 4096], P(None, None, None, 'col'), may hold values from -6 to 6
- layer_in: bfloat16 [2, 6, 64, 4096], P(None, None, None, 'row'), may hold values from -1 to 1
- h_prev: bfloat16 [2, 6, 64, 4096], P(None, None, None, 'row'), may hold values from -1 to 1
- top_grad: float32 [6, 64, 4096], P(None, None, 'col'), may hold values from -40 to 40
Outputs:
- w_rec_grad: bfloat16 [2, 4096, 4, 4096], P(None, 'row', None, 'col')
- w_in_grad: bfloat16 [2, 4096, 4, 4096], P(None, 'row', None, 'col')
- input_grad: float32 [6, 64, 4096], P(None, None, 'col')
The draws below stay inside these ranges and needn't reach their ends.
Inputs may be any that keep to these rules, and one draw needn't show every extreme that they name: `gate_pre`: dimension 3 holds the input, forget, candidate and output gates in that order.
All inputs are finite; a program needn't handle non-finite values.
Results may differ from the reference program's by a relative error of at most 0.0051.
Values sent between devices are 32-bit elements; how exact they have to be, the bound alone decides.
A program may use at most 128 MiB of HBM per device.

```python
import math
import jax
import jax.numpy as jnp
from jax import lax

WIDTH = 4096
LAYERS = 2
STEPS = 6
BATCH = 64


def draw_gate_pre(key, part):
    first, second = jax.random.split(jax.random.fold_in(key, 11), 2)
    shape = (LAYERS, STEPS, BATCH, 4, WIDTH)
    noise = jax.random.normal(first, shape, jnp.float32)
    offset = jax.random.uniform(second, (LAYERS, 1, 1, 1, WIDTH), jnp.float32, -1.0, 5.0)
    chosen = (jnp.arange(4) == 1).reshape(1, 1, 1, 4, 1)
    values = jnp.where(chosen, offset + 0.7 * noise, 1.5 * noise)
    return jnp.clip(values, -8.0, 8.0)


def draw_top_grad(key, part):
    first, second, third = jax.random.split(jax.random.fold_in(key, 23), 3)
    shape = (STEPS, BATCH, WIDTH)
    phases = jax.random.uniform(first, (2,), jnp.float32, 0.0, 2.0 * math.pi)
    where_unit = jnp.arange(WIDTH).astype(jnp.float32) / WIDTH
    envelope = 1.2 * jnp.sin(2.0 * math.pi * where_unit + phases[0]) + 0.6 * jnp.sin(6.0 * math.pi * where_unit + phases[1])
    factor = 2.0 * jnp.exp(envelope)
    base = jax.random.normal(second, shape, jnp.float32)
    return jnp.clip(base * factor, -40.0, 40.0)


def steps_of(rng, shape, shards, smallest, largest):
    level = 1.0
    for axis_at, blocks in shards:
        heights = jax.random.uniform(jax.random.fold_in(jax.random.fold_in(rng, 6), axis_at), (blocks,), jnp.float32, smallest / len(shards), largest / len(shards))
        level = level * jnp.repeat(jnp.exp(heights), shape[axis_at] // blocks).reshape((-1,) + (1,) * (len(shape) - 1 - axis_at))
    return level


def scatter_about(stream_key, extent, deviation, bound, shards=(), kind=jnp.bfloat16):
    array = deviation * jax.random.normal(stream_key, extent, jnp.float32)
    if shards:
        array = array * steps_of(stream_key, extent, shards, -0.22, 0.18)
    return jnp.clip(array, -bound, bound).astype(kind)


def setup_inputs(seed: int = 0) -> dict:
    streams_of = jax.random.split(jax.random.key(seed), 8)
    return {
        "w_rec": scatter_about(streams_of[0], (LAYERS, WIDTH, 4, WIDTH), WIDTH ** -0.5, 0.09375, ((1, 4), (3, 8))),
        "w_in": scatter_about(streams_of[1], (LAYERS, WIDTH, 4, WIDTH), WIDTH ** -0.5, 0.09375, ((1, 4), (3, 8))),
        "gate_pre": draw_gate_pre(jax.random.fold_in(streams_of[7], 71), 0),
        "cells": scatter_about(streams_of[3], (LAYERS, STEPS + 1, BATCH, WIDTH), 1.0, 6.0, ((3, 8),), jnp.float32),
        "layer_in": jnp.clip(jax.random.uniform(streams_of[4], (LAYERS, STEPS, BATCH, WIDTH), jnp.float32, -1.0, 1.0) * steps_of(streams_of[4], (LAYERS, STEPS, BATCH, WIDTH), ((3, 4),), -0.4, 0.0), -1.0, 1.0).astype(jnp.bfloat16),
        "h_prev": jnp.clip(jax.random.uniform(streams_of[5], (LAYERS, STEPS, BATCH, WIDTH), jnp.float32, -1.0, 1.0) * steps_of(streams_of[5], (LAYERS, STEPS, BATCH, WIDTH), ((3, 4),), -0.4, 0.0), -1.0, 1.0).astype(jnp.bfloat16),
        "top_grad": draw_top_grad(jax.random.fold_in(streams_of[7], 71), 0),
    }


def cell_backward(preact, cell_prev, cell_now, hid_grad, cell_carry):
    in_gate = jax.nn.sigmoid(preact[:, 0])
    forget = jax.nn.sigmoid(preact[:, 1])
    cand_gate = jnp.tanh(preact[:, 2])
    out_gate = jax.nn.sigmoid(preact[:, 3])
    tanh_cell = jnp.tanh(cell_now)
    cell_grad = cell_carry + hid_grad * out_gate * (1.0 - tanh_cell * tanh_cell)
    grad_in = cell_grad * cand_gate * in_gate * (1.0 - in_gate)
    grad_forget = cell_grad * cell_prev * forget * (1.0 - forget)
    grad_cand = cell_grad * in_gate * (1.0 - cand_gate * cand_gate)
    grad_out = hid_grad * tanh_cell * out_gate * (1.0 - out_gate)
    gate_grads = jnp.stack([grad_in, grad_forget, grad_cand, grad_out], axis=1).astype(jnp.bfloat16)
    return (gate_grads, cell_grad * forget)

def reference(w_rec, w_in, gate_pre, cells, layer_in, h_prev, top_grad):
    incoming = top_grad
    rec_grads = [None] * LAYERS
    in_grads = [None] * LAYERS
    sumsq = jnp.zeros((), jnp.float32)
    for layer in range(LAYERS - 1, -1, -1):
        rec_flat = w_rec[layer].reshape(WIDTH, 4 * WIDTH)

        def advance(carry, inputs, rec_flat=rec_flat):
            rec_carry, cell_carry = carry
            preact, cell_prev, cell_now, outside = inputs
            gate_grads, cell_next = cell_backward(preact, cell_prev, cell_now, outside + rec_carry, cell_carry)
            recurrent = jnp.dot(gate_grads.reshape(BATCH, 4 * WIDTH), rec_flat.T, preferred_element_type=jnp.float32)
            return ((recurrent, cell_next), gate_grads)
        zeros = jnp.zeros((BATCH, WIDTH), jnp.float32)
        carried, stacked = lax.scan(advance, (zeros, zeros), (gate_pre[layer], cells[layer, :STEPS], cells[layer, 1:], incoming), reverse=True)
        flat = stacked.reshape(STEPS * BATCH, 4 * WIDTH)
        incoming = jnp.dot(flat, w_in[layer].reshape(WIDTH, 4 * WIDTH).T, preferred_element_type=jnp.float32).reshape(STEPS, BATCH, WIDTH)
        raw_rec = jnp.dot(h_prev[layer].reshape(STEPS * BATCH, WIDTH).T, flat, preferred_element_type=jnp.float32)
        raw_in = jnp.dot(layer_in[layer].reshape(STEPS * BATCH, WIDTH).T, flat, preferred_element_type=jnp.float32)
        sumsq = sumsq + jnp.sum(raw_rec * raw_rec) + jnp.sum(raw_in * raw_in)
        rec_grads[layer] = raw_rec
        in_grads[layer] = raw_in
    scale = 1.0 / jnp.maximum(jnp.sqrt(sumsq / (8.0 * LAYERS * WIDTH * WIDTH)), 0.05)
    w_rec_grad = jnp.stack([(rec_grads[layer] * scale).reshape(WIDTH, 4, WIDTH) for layer in range(LAYERS)]).astype(jnp.bfloat16)
    w_in_grad = jnp.stack([(in_grads[layer] * scale).reshape(WIDTH, 4, WIDTH) for layer in range(LAYERS)]).astype(jnp.bfloat16)
    return (w_rec_grad, w_in_grad, incoming)
```

```python
import functools

import jax
import jax.numpy as jnp
from jax import lax
from jax.experimental import pallas as pl
from jax.experimental.pallas import tpu as pltpu
from jax.sharding import PartitionSpec as P

MESH = pl.DeviceIdType.MESH
F32 = jnp.float32
BF16 = jnp.bfloat16
VMEM_BYTES = 60 * 1024 * 1024


def contract(left, right, dims):
    return lax.dot_general(left, right, ((dims[0], dims[1]), ((), ())), preferred_element_type=F32)


def tile_of(size, limit):
    while size % limit:
        limit //= 2
    return limit


def recurrence_kernel(
    rows, ratio, layers, steps,
    w_rec, w_in, gate_pre, cells, top_grad, gram,
    flats, input_grad, squares,
    rec_w, in_w, fac, carry, sq_acc, part, recv_a, acc, recv_b, gat, sq_mine, sq_a, sq_sum, sq_b,
    w_sem, sa, ra, sb, rb, sc, rc, qsa, qra, qsb, qrb,
):
    top = layers - 1
    diagonals = steps + top
    batch, units = top_grad.shape[1:]
    piece = batch // rows
    kind_in = layers
    row = lax.axis_index("row")
    col = lax.axis_index("col")
    deep, half = col // ratio, col % ratio

    def loads(layer):
        return (
            pltpu.make_async_copy(w_rec.at[layer], rec_w.at[layer], w_sem.at[0, layer]),
            pltpu.make_async_copy(w_in.at[layer], in_w.at[layer], w_sem.at[1, layer]),
        )

    for layer in range(top, -1, -1):
        for copy in loads(layer):
            copy.start()

    plane = [(dr, dh) for dr in range(rows) for dh in range(ratio)][1:]
    slot_of = {offset: index for index, offset in enumerate(plane)}

    def plane_peer(dr, dh):
        return ((row + dr) % rows, deep * ratio + (half + dh) % ratio)

    def line_peer(dz):
        return (row, ((deep + dz) % rows) * ratio + half)

    def row_peer(dq):
        return ((row + dq) % rows, col)

    barrier = pltpu.get_barrier_semaphore()
    for offset in plane:
        pl.semaphore_signal(barrier, inc=1, device_id=plane_peer(*offset), device_id_type=MESH)
    for dz in range(1, rows):
        pl.semaphore_signal(barrier, inc=1, device_id=line_peer(dz), device_id_type=MESH)
    pl.semaphore_wait(barrier, len(plane) + rows - 1)

    def remote(src, dst, send, recv, device):
        return pltpu.make_async_remote_copy(
            src_ref=src, dst_ref=dst, send_sem=send, recv_sem=recv, device_id=device, device_id_type=MESH
        )

    def quarter(index):
        return pl.ds(pl.multiple_of(index * piece, piece), piece)

    def lanes(index, size):
        return pl.ds(pl.multiple_of(index * size, size), size)

    def copy_a(kind, d, offset):
        dr, dh = offset
        slot = slot_of[offset]
        src = part.at[kind, d, quarter((row + dr) % rows), lanes((half + dh) % ratio, units)]
        return remote(src, recv_a.at[kind, d, slot], sa.at[kind, d, slot], ra.at[kind, d, slot], plane_peer(dr, dh))

    def copy_b(kind, d, dz):
        src = acc.at[kind, d, (deep + dz) % rows]
        return remote(src, recv_b.at[kind, d, dz - 1], sb.at[kind, d, dz - 1], rb.at[kind, d, dz - 1], line_peer(dz))

    def copy_c(kind, d, dq):
        spot = gat.at[kind, d, quarter(row)]
        return remote(spot, spot, sc.at[kind, d, dq - 1], rc.at[kind, d, dq - 1], row_peer(dq))

    def start_a(kind, d):
        for offset in plane:
            copy_a(kind, d, offset).start()

    def finish_a(kind, d):
        for offset in plane:
            copy_a(kind, d, offset).wait_recv()
        for dr in range(rows):
            value = None
            for dh in range(ratio):
                if dr == 0 and dh == 0:
                    new = part[kind, d, quarter(row), lanes(half, units)]
                else:
                    new = recv_a[kind, d, slot_of[(dr, dh)]]
                value = new if value is None else value + new
            acc[kind, d, (row - dr + rows) % rows] = value
        for dz in range(1, rows):
            copy_b(kind, d, dz).start()

    def finish_b(kind, d):
        value = acc[kind, d, deep]
        for dz in range(1, rows):
            copy_b(kind, d, dz).wait_recv()
            value = value + recv_b[kind, d, dz - 1]
        gat[kind, d, quarter(row)] = value
        for dq in range(1, rows):
            copy_c(kind, d, dq).start()

    def finish_c(kind, d):
        for dq in range(1, rows):
            spot = gat.at[kind, d, quarter((row - dq + rows) % rows)]
            remote(spot, spot, sc.at[kind, d, dq - 1], rc.at[kind, d, dq - 1], row_peer(dq)).wait_recv()

    def sent(kind, d):
        for offset in plane:
            copy_a(kind, d, offset).wait_send()
        for dz in range(1, rows):
            copy_b(kind, d, dz).wait_send()
        for dq in range(1, rows):
            copy_c(kind, d, dq).wait_send()

    def step_of(layer, d):
        return steps - 1 - d + top - layer

    def active(layer, d):
        return (d >= top - layer) & (d <= top - layer + steps - 1)

    def feeds(layer, d):
        first = top - layer - 1 if layer < top else 0
        return (d >= first) & (d <= top - layer + steps - 2)

    chunk = 16

    def factors(layer, step):
        def body(index, _):
            at = pl.ds(pl.multiple_of(index * chunk, chunk), chunk)
            in_gate = jax.nn.sigmoid(gate_pre[layer, step, 0, at, :])
            forget = jax.nn.sigmoid(gate_pre[layer, step, 1, at, :])
            cand = jnp.tanh(gate_pre[layer, step, 2, at, :])
            out_gate = jax.nn.sigmoid(gate_pre[layer, step, 3, at, :])
            tanh_cell = jnp.tanh(cells[layer, step + 1, at, :])
            fac[layer, 0, at, :] = out_gate * (1.0 - tanh_cell * tanh_cell)
            fac[layer, 1, at, :] = cand * in_gate * (1.0 - in_gate)
            fac[layer, 2, at, :] = cells[layer, step, at, :] * forget * (1.0 - forget)
            fac[layer, 3, at, :] = in_gate * (1.0 - cand * cand)
            fac[layer, 4, at, :] = tanh_cell * out_gate * (1.0 - out_gate)
            fac[layer, 5, at, :] = forget
            return 0

        lax.fori_loop(0, batch // chunk, body, 0)

    def cell(layer, d, step):
        def body(index, _):
            at = pl.ds(pl.multiple_of(index * chunk, chunk), chunk)
            out_at = pl.ds(pl.multiple_of(step * batch + index * chunk, chunk), chunk)
            if layer == top:
                hid = top_grad[step, at, :] + gat[layer, d, at, :]
            else:
                hid = gat[layer, d, at, :]
            grad = carry[layer, at, :] + hid * fac[layer, 0, at, :]
            for gate in range(3):
                flats[layer, out_at, gate * units:(gate + 1) * units] = (grad * fac[layer, gate + 1, at, :]).astype(BF16)
            flats[layer, out_at, 3 * units:] = (hid * fac[layer, 4, at, :]).astype(BF16)
            carry[layer, at, :] = grad * fac[layer, 5, at, :]
            return 0

        lax.fori_loop(0, batch // chunk, body, 0)

    outs = part.shape[-1]
    wide = tile_of(outs, 256)

    def product(weights, layer, step, kind, d, add):
        at = pl.ds(pl.multiple_of(step * batch, batch), batch)

        def body(index, _):
            spot = pl.ds(pl.multiple_of(index * wide, wide), wide)
            value = part[kind, d, :, spot] if add else None
            for gate in range(4):
                new = contract(flats[layer, at, gate * units:(gate + 1) * units], weights[layer, gate, spot, :], ((1,), (1,)))
                value = new if value is None else value + new
            part[kind, d, :, spot] = value
            return 0

        lax.fori_loop(0, outs // wide, body, 0)

    def grams(layer, step):
        at = pl.ds(pl.multiple_of(step * batch, batch), batch)

        def body(other, _):
            there = pl.ds(pl.multiple_of(other * batch, batch), batch)
            both = contract(flats[layer, at, :], flats[layer, there, :], ((1,), (1,)))
            weight = jnp.where(other == step, 1.0, 2.0).astype(F32)
            sq_acc[...] = sq_acc[...] + weight * (both * gram[layer, step, other])
            return 0

        lax.fori_loop(step, steps, body, 0)

    carry[...] = jnp.zeros_like(carry)
    sq_acc[...] = jnp.zeros_like(sq_acc)
    gat[top, diagonals] = jnp.zeros(gat.shape[2:], F32)
    factors(top, steps - 1)

    def diagonal(d, _):
        for layer in range(top, -1, -1):
            step = step_of(layer, d)

            @pl.when(active(layer, d))
            def _(layer=layer, step=step):
                before = d - 1
                if layer == top:
                    before = jnp.where(d == 0, diagonals, d - 1)

                    @pl.when(d > 0)
                    def _():
                        finish_c(layer, d - 1)
                else:
                    finish_c(layer, d - 1)
                cell(layer, before, step)

                @pl.when(d == top - layer)
                def _():
                    for copy in loads(layer):
                        copy.wait()

            @pl.when(feeds(layer, d))
            def _(layer=layer, step=step):
                if layer == top:
                    product(rec_w, layer, step, layer, d, False)
                else:
                    product(in_w, layer + 1, step_of(layer + 1, d), layer, d, False)

                    @pl.when(step < steps)
                    def _():
                        product(rec_w, layer, step, layer, d, True)

                start_a(layer, d)

        for layer in range(top, -1, -1):
            @pl.when(feeds(layer, d))
            def _(layer=layer):
                finish_a(layer, d)

        @pl.when(d >= top + 1)
        def _():
            finish_b(kind_in, d - 1)

        @pl.when(d >= top)
        def _():
            product(in_w, 0, step_of(0, d), kind_in, d, False)
            start_a(kind_in, d)

        for layer in range(top, -1, -1):
            @pl.when(active(layer, d))
            def _(layer=layer):
                grams(layer, step_of(layer, d))

            @pl.when(active(layer, d + 1))
            def _(layer=layer):
                factors(layer, step_of(layer, d + 1))

        @pl.when(d == diagonals - 1)
        def _():
            sq_mine[...] = jnp.full(sq_mine.shape, jnp.sum(sq_acc[...]), F32)
            for offset in plane:
                sq_copy_a(offset).start()

        for layer in range(top, -1, -1):
            @pl.when(feeds(layer, d))
            def _(layer=layer):
                finish_b(layer, d)

        @pl.when(d >= top)
        def _():
            finish_a(kind_in, d)

        return 0

    def sq_copy_a(offset):
        slot = slot_of[offset]
        return remote(sq_mine, sq_a.at[slot], qsa.at[slot], qra.at[slot], plane_peer(*offset))

    def sq_copy_b(dz):
        return remote(sq_sum, sq_b.at[dz - 1], qsb.at[dz - 1], qrb.at[dz - 1], line_peer(dz))

    lax.fori_loop(0, diagonals, diagonal, 0)

    value = sq_mine[...]
    for offset in plane:
        sq_copy_a(offset).wait_recv()
        value = value + sq_a[slot_of[offset]]
    sq_sum[...] = value
    for dz in range(1, rows):
        sq_copy_b(dz).start()
    finish_b(kind_in, diagonals - 1)
    value = sq_sum[...]
    for dz in range(1, rows):
        sq_copy_b(dz).wait_recv()
        value = value + sq_b[dz - 1]
    squares[...] = value

    def collect(d, _):
        finish_c(kind_in, d)
        input_grad[step_of(0, d)] = gat[kind_in, d]
        sent(kind_in, d)
        return 0

    lax.fori_loop(top, diagonals, collect, 0)

    def settle(d, _):
        for layer in range(layers):
            @pl.when(feeds(layer, d))
            def _(layer=layer):
                sent(layer, d)

        return 0

    lax.fori_loop(0, diagonals, settle, 0)
    for offset in plane:
        sq_copy_a(offset).wait_send()
    for dz in range(1, rows):
        sq_copy_b(dz).wait_send()


def recurrence(w_rec, w_in, gate_pre, cells, top_grad, gram):
    rows, cols = lax.axis_size("row"), lax.axis_size("col")
    ratio = cols // rows
    layers, _, row_units, units = w_rec.shape
    steps, batch, _ = top_grad.shape
    diagonals = steps + layers - 1
    piece = batch // rows
    kinds = layers + 1
    group = rows * ratio - 1
    dma = pltpu.SemaphoreType.DMA
    vmem = lambda *shape: pltpu.VMEM(shape, F32)
    in_vmem = pl.BlockSpec(memory_space=pltpu.VMEM)
    in_any = pl.BlockSpec(memory_space=pl.ANY)
    return pl.pallas_call(
        functools.partial(recurrence_kernel, rows, ratio, layers, steps),
        out_shape=[
            jax.ShapeDtypeStruct((layers, steps * batch, 4 * units), BF16),
            jax.ShapeDtypeStruct((steps, batch, units), F32),
            jax.ShapeDtypeStruct((8, 128), F32),
        ],
        in_specs=[in_any, in_any, in_vmem, in_vmem, in_vmem, in_vmem],
        out_specs=[in_vmem] * 3,
        scratch_shapes=[
            pltpu.VMEM((layers, 4, row_units, units), BF16), pltpu.VMEM((layers, 4, row_units, units), BF16),
            vmem(layers, 6, batch, units), vmem(layers, batch, units), vmem(batch, batch),
            vmem(kinds, diagonals, batch, row_units), vmem(kinds, diagonals, group, piece, units),
            vmem(kinds, diagonals, rows, piece, units), vmem(kinds, diagonals, rows - 1, piece, units),
            vmem(kinds, diagonals + 1, batch, units),
            vmem(8, 128), vmem(group, 8, 128), vmem(8, 128), vmem(rows - 1, 8, 128),
            dma((2, layers)),
            dma((kinds, diagonals, group)), dma((kinds, diagonals, group)),
            dma((kinds, diagonals, rows - 1)), dma((kinds, diagonals, rows - 1)),
            dma((kinds, diagonals, rows - 1)), dma((kinds, diagonals, rows - 1)),
            dma((group,)), dma((group,)), dma((rows - 1,)), dma((rows - 1,)),
        ],
        compiler_params=pltpu.CompilerParams(collective_id=0, has_side_effects=True, vmem_limit_bytes=VMEM_BYTES),
        name="recurrence",
    )(w_rec, w_in, gate_pre, cells, top_grad, gram)


def weight_kernel(entries, squares, h_prev, layer_in, flats, rec_out, in_out, stage):
    scale = 1.0 / jnp.maximum(jnp.sqrt(squares[...] / entries), 0.05)
    tall, units = rec_out.shape[1], rec_out.shape[3]
    scale = jnp.broadcast_to(scale[:1, :1], (tall, units))
    for source, out in ((h_prev, rec_out), (layer_in, in_out)):
        left = source[0].T
        for gate in range(4):
            value = contract(left, flats[0, :, gate * units:(gate + 1) * units], ((1,), (0,))) * scale
            for lane in range(units // 128):
                stage[lane, pl.ds(gate, tall, stride=4), :] = value[:, lane * 128:(lane + 1) * 128]
        for lane in range(units // 128):
            out[0, :, :, lane * 128:(lane + 1) * 128] = stage[lane].astype(BF16).reshape(tall, 4, 128)


def weight_grads(squares, h_prev, layer_in, flats, entries):
    layers, tokens, row_units = h_prev.shape
    units = flats.shape[2] // 4
    tall = tile_of(row_units, 128)
    source = pl.BlockSpec((1, tokens, tall), lambda layer, tile: (layer, 0, tile))
    target = pl.BlockSpec((1, tall, 4, units), lambda layer, tile: (layer, tile, 0, 0))
    shape = jax.ShapeDtypeStruct((layers, row_units, 4, units), BF16)
    return pl.pallas_call(
        functools.partial(weight_kernel, entries),
        grid=(layers, row_units // tall),
        out_shape=[shape, shape],
        in_specs=[
            pl.BlockSpec((8, 128), lambda layer, tile: (0, 0)),
            source, source,
            pl.BlockSpec((1, tokens, 4 * units), lambda layer, tile: (layer, 0, 0)),
        ],
        out_specs=[target, target],
        scratch_shapes=[pltpu.VMEM((units // 128, 4 * tall, 128), F32)],
        name="weight_grads",
    )(squares, h_prev, layer_in, flats)


def local(w_rec, w_in, gate_pre, cells, layer_in, h_prev, top_grad):
    layers, row_units = w_rec.shape[:2]
    steps, batch, units = top_grad.shape
    rec_in = h_prev.reshape(layers, steps * batch, row_units)
    lay_in = layer_in.reshape(layers, steps * batch, row_units)
    gram = jnp.stack([
        contract(rec_in[layer], rec_in[layer], ((1,), (1,))) + contract(lay_in[layer], lay_in[layer], ((1,), (1,)))
        for layer in range(layers)
    ])
    gram = gram.reshape(layers, steps, batch, steps, batch).transpose(0, 1, 3, 2, 4)
    flats, input_grad, squares = recurrence(
        w_rec.transpose(0, 2, 1, 3), w_in.transpose(0, 2, 1, 3), gate_pre.transpose(0, 1, 3, 2, 4), cells, top_grad, gram
    )
    entries = 2.0 * layers * (row_units * lax.axis_size("row")) * (4 * units * lax.axis_size("col"))
    rec_grad, in_grad = weight_grads(squares, rec_in, lay_in, flats, entries)
    return (rec_grad, in_grad, input_grad)


def solution(mesh):
    placed = (
        P(None, "row", None, "col"),
        P(None, "row", None, "col"),
        P(None, None, None, None, "col"),
        P(None, None, None, "col"),
        P(None, None, None, "row"),
        P(None, None, None, "row"),
        P(None, None, "col"),
    )
    return jax.shard_map(
        local,
        mesh=mesh,
        in_specs=placed,
        out_specs=(P(None, "row", None, "col"), P(None, "row", None, "col"), P(None, None, "col")),
        check_vma=False,
    )
```

```python
import functools

import jax
import jax.numpy as jnp
from jax import lax
from jax.experimental import pallas as pl
from jax.experimental.pallas import tpu as pltpu
from jax.sharding import PartitionSpec as P

MESH = pl.DeviceIdType.MESH
F32 = jnp.float32
BF16 = jnp.bfloat16
VMEM_BYTES = 60 * 1024 * 1024


def contract(left, right, dims):
    return lax.dot_general(left, right, ((dims[0], dims[1]), ((), ())), preferred_element_type=F32)


def tile_of(size, limit):
    while size % limit:
        limit //= 2
    return limit


def recurrence_kernel(
    rows, cores, ratio, layers, steps,
    w_rec, w_in, gate_pre_any, cells_any, top_grad_any, h_prev_any, layer_in_any,
    flats, input_grad, squares,
    rec_w, in_w, raw, fold, gate_pre, cells, top_grad, h_prev, layer_in, fac, carry, sq_acc, part, recv_a, acc, recv_r, recv_b, gat, sq_mine, sq_a, sq_sum, sq_b,
    w_sem, e_sem, sa, ra, sr, rr, sb, rb, sc, rc, qsa, qra, qsb, qrb,
):
    top = layers - 1
    diagonals = steps + top
    batch, units = top_grad_any.shape[1:]
    piece = batch // rows
    kind_in = layers
    row = lax.axis_index("row")
    col = lax.axis_index("col")
    deep, half = col // ratio, col % ratio
    lots = rows // cores
    lot, core = row // cores, row % cores
    inside = core == deep % cores

    def load(which, layer):
        return pltpu.make_async_copy((w_rec, w_in)[which].at[layer], raw.at[which], w_sem.at[which])

    def move(src, dst, at, index):
        return pltpu.make_async_copy(src.at[at], dst.at[at], e_sem.at[index])

    late = steps - 1
    early = [
        move(gate_pre_any, gate_pre, (top, late), 0),
        move(cells_any, cells, top, 1),
        move(top_grad_any, top_grad, slice(None), 2),
    ]
    rest = [move(gate_pre_any, gate_pre, (top, slice(0, late)), 3)] if late else []
    for layer in range(top):
        rest.append(move(gate_pre_any, gate_pre, layer, 4 + 2 * layer))
        rest.append(move(cells_any, cells, layer, 5 + 2 * layer))
    rest.append(move(h_prev_any, h_prev, slice(None), 4 + 2 * top))
    rest.append(move(layer_in_any, layer_in, slice(None), 5 + 2 * top))
    for copy in early:
        copy.start()
    for which in range(2):
        load(which, top).start()
    for copy in rest:
        copy.start()

    plane = [(dr, dh) for dr in range(rows) for dh in range(ratio)][1:]
    slot_of = {offset: index for index, offset in enumerate(plane)}

    def plane_peer(dr, dh):
        return ((row + dr) % rows, deep * ratio + (half + dh) % ratio)

    def line_peer(dz):
        return (row, ((deep + dz) % rows) * ratio + half)

    def row_peer(dq):
        return ((row + dq) % rows, col)

    barrier = pltpu.get_barrier_semaphore()
    for offset in plane:
        pl.semaphore_signal(barrier, inc=1, device_id=plane_peer(*offset), device_id_type=MESH)
    for dz in range(1, rows):
        pl.semaphore_signal(barrier, inc=1, device_id=line_peer(dz), device_id_type=MESH)
    for dz in range(rows):
        source = (lot * cores + deep % cores, ((deep - dz + rows) % rows) * ratio + half)
        if dz:
            pl.semaphore_signal(barrier, inc=1, device_id=source, device_id_type=MESH)
        else:
            @pl.when(jnp.logical_not(inside))
            def _(source=source):
                pl.semaphore_signal(barrier, inc=1, device_id=source, device_id_type=MESH)

    pl.semaphore_wait(barrier, len(plane) + rows - 1 + rows - jnp.where(inside, 1, 0))

    def remote(src, dst, send, recv, device):
        return pltpu.make_async_remote_copy(
            src_ref=src, dst_ref=dst, send_sem=send, recv_sem=recv, device_id=device, device_id_type=MESH
        )

    def quarter(index):
        return pl.ds(pl.multiple_of(index * piece, piece), piece)

    def lanes(index, size):
        return pl.ds(pl.multiple_of(index * size, size), size)

    turns = [(dx, dg) for dx in list(range(1, lots)) + [0] for dg in list(range(1, cores)) + [0]]

    def block_of(dx, dg):
        return ((lot + dx) % lots) * cores + (core + dg) % cores

    def copy_a(kind, d, dh, dx, dg):
        src = part.at[kind, d, quarter(block_of(dx, dg)), lanes((half + dh) % ratio, units)]
        spot = (kind, d, dh - 1, dx, dg)
        return remote(src, recv_a.at[spot], sa.at[spot], ra.at[spot], plane_peer(0, dh))

    def copy_r(kind, d, dx, dg):
        spot = (kind, d, dx - 1, dg)
        return remote(acc.at[kind, d, dx, dg], recv_r.at[spot], sr.at[spot], rr.at[spot], (block_of(dx, 0), col))

    def origin(dx):
        return block_of(lots - dx, 0)

    def copy_b(kind, d, dx, dg):
        src = recv_r.at[kind, d, dx - 1, dg] if dx else acc.at[kind, d, 0, dg]
        slot = (origin(dx) - deep + rows) % rows
        peer = (block_of(0, dg), origin(dx) * ratio + half)
        return remote(src, recv_b.at[kind, d, slot], sb.at[kind, d, dx, dg], rb.at[kind, d, slot], peer)

    def copy_c(kind, d, dq):
        spot = gat.at[kind, d, quarter(row)]
        return remote(spot, spot, sc.at[kind, d, dq - 1], rc.at[kind, d, dq - 1], row_peer(dq))

    def start_a(kind, d, dh):
        for dx, dg in turns:
            copy_a(kind, d, dh, dx, dg).start()

    def finish_a(kind, d):
        for dx, dg in turns:
            value = part[kind, d, quarter(block_of(dx, dg)), lanes(half, units)]
            for dh in range(1, ratio):
                copy_a(kind, d, dh, dx, dg).wait_recv()
                value = value + recv_a[kind, d, dh - 1, dx, dg]
            if dx:
                acc[kind, d, dx, dg] = value
                copy_r(kind, d, dx, dg).start()
            elif dg:
                acc[kind, d, 0, dg] = value
                copy_b(kind, d, 0, dg).start()
            else:
                home = row == deep

                @pl.when(home)
                def _():
                    recv_b[kind, d, 0] = value

                @pl.when(jnp.logical_not(home))
                def _():
                    acc[kind, d, 0, 0] = value
                    copy_b(kind, d, 0, 0).start()

    def finish_r(kind, d):
        for dx in range(1, lots):
            for dg in list(range(1, cores)) + [0]:
                copy_r(kind, d, dx, dg).wait_recv()
                if dg:
                    copy_b(kind, d, dx, dg).start()
                else:
                    home = origin(dx) == deep

                    @pl.when(home)
                    def _():
                        recv_b[kind, d, 0] = recv_r[kind, d, dx - 1, 0]

                    @pl.when(jnp.logical_not(home))
                    def _():
                        copy_b(kind, d, dx, 0).start()

    def source_of(dz):
        return (lot * cores + deep % cores, ((deep - dz + rows) % rows) * ratio + half)

    def arrival(kind, d, dz):
        return remote(acc.at[kind, d, 0, 0], recv_b.at[kind, d, dz], sb.at[kind, d, 0, 0], rb.at[kind, d, dz], source_of(dz))

    def finish_b(kind, d):
        @pl.when(jnp.logical_not(inside))
        def _():
            arrival(kind, d, 0).wait_recv()

        for dz in range(1, rows):
            arrival(kind, d, dz).wait_recv()
        value = recv_b[kind, d, 0]
        for dz in range(1, rows):
            value = value + recv_b[kind, d, dz]
        gat[kind, d, quarter(row)] = value
        for dq in range(1, rows):
            copy_c(kind, d, dq).start()

    def finish_c(kind, d):
        for dq in range(1, rows):
            spot = gat.at[kind, d, quarter((row - dq + rows) % rows)]
            remote(spot, spot, sc.at[kind, d, dq - 1], rc.at[kind, d, dq - 1], row_peer(dq)).wait_recv()

    def sent(kind, d):
        for dx, dg in turns:
            for dh in range(1, ratio):
                copy_a(kind, d, dh, dx, dg).wait_send()
            if dx:
                copy_r(kind, d, dx, dg).wait_send()
            if dg:
                copy_b(kind, d, dx, dg).wait_send()
            else:
                @pl.when(origin(dx) != deep)
                def _(dx=dx):
                    copy_b(kind, d, dx, 0).wait_send()

        for dq in range(1, rows):
            copy_c(kind, d, dq).wait_send()

    def step_of(layer, d):
        return steps - 1 - d + top - layer

    def active(layer, d):
        return both(d >= top - layer, d <= top - layer + steps - 1)

    def feeds(layer, d):
        first = top - layer - 1 if layer < top else 0
        return both(d >= first, d <= top - layer + steps - 2)

    chunk = 16

    def factors(layer, step):
        def body(index, _):
            at = pl.ds(pl.multiple_of(index * chunk, chunk), chunk)
            in_gate = jax.nn.sigmoid(gate_pre[layer, step, at, 0, :])
            forget = jax.nn.sigmoid(gate_pre[layer, step, at, 1, :])
            cand = jnp.tanh(gate_pre[layer, step, at, 2, :])
            out_gate = jax.nn.sigmoid(gate_pre[layer, step, at, 3, :])
            tanh_cell = jnp.tanh(cells[layer, step + 1, at, :])
            fac[layer, 0, at, :] = out_gate * (1.0 - tanh_cell * tanh_cell)
            fac[layer, 1, at, :] = cand * in_gate * (1.0 - in_gate)
            fac[layer, 2, at, :] = cells[layer, step, at, :] * forget * (1.0 - forget)
            fac[layer, 3, at, :] = in_gate * (1.0 - cand * cand)
            fac[layer, 4, at, :] = tanh_cell * out_gate * (1.0 - out_gate)
            fac[layer, 5, at, :] = forget
            return 0

        lax.fori_loop(0, batch // chunk, body, 0)

    def cell(layer, d, step):
        def body(index, _):
            at = pl.ds(pl.multiple_of(index * chunk, chunk), chunk)
            out_at = pl.ds(pl.multiple_of(step * batch + index * chunk, chunk), chunk)
            if layer == top:
                hid = top_grad[step, at, :] + gat[layer, d, at, :]
            else:
                hid = gat[layer, d, at, :]
            grad = carry[layer, at, :] + hid * fac[layer, 0, at, :]
            for gate in range(3):
                flats[layer, out_at, gate * units:(gate + 1) * units] = (grad * fac[layer, gate + 1, at, :]).astype(BF16)
            flats[layer, out_at, 3 * units:] = (hid * fac[layer, 4, at, :]).astype(BF16)
            carry[layer, at, :] = grad * fac[layer, 5, at, :]
            return 0

        lax.fori_loop(0, batch // chunk, body, 0)

    row_units = part.shape[-1]

    def rows_of(step):
        return pl.ds(step * batch if isinstance(step, int) else pl.multiple_of(step * batch, batch), batch)

    def product(weights, layer, step, kind, d, dh, add):
        at = rows_of(step)
        spot = lanes((half + dh) % ratio, units)
        value = part[kind, d, :, spot] if add else None
        for gate in range(4):
            new = contract(flats[layer, at, gate * units:(gate + 1) * units], weights[layer, gate, :, spot], ((1,), (0,)))
            value = new if value is None else value + new
        part[kind, d, :, spot] = value

    def send_product(weights, layer, step, kind, d, add):
        for dh in list(range(1, ratio)) + [0]:
            product(weights, layer, step, kind, d, dh, add)
            if dh:
                start_a(kind, d, dh)

    tall = 128

    def unfold(which, weights, layer):
        def body(index, _):
            at = pl.ds(pl.multiple_of(index * tall, tall), tall)
            for lane in range(units // 128):
                span = slice(lane * 128, (lane + 1) * 128)
                fold[lane] = raw[which, at, :, span].astype(F32).reshape(4 * tall, 128)
            for lane in range(units // 128):
                span = slice(lane * 128, (lane + 1) * 128)
                for gate in range(4):
                    weights[layer, gate, span, at] = fold[lane, pl.ds(gate, tall, stride=4), :].astype(BF16).T
            return 0

        lax.fori_loop(0, row_units // tall, body, 0)

    tokens = steps * batch

    def grams(layer, step):
        at = rows_of(step)
        both = contract(flats[layer, at, :], flats[layer], ((1,), (1,)))
        outer = contract(h_prev[layer, at, :], h_prev[layer], ((1,), (1,)))
        outer = outer + contract(layer_in[layer, at, :], layer_in[layer], ((1,), (1,)))
        other = lax.broadcasted_iota(jnp.int32, (batch, tokens), 1)
        first = step * batch
        weight = jnp.where((other >= first) & (other < first + batch), 1.0, 2.0).astype(F32)
        sq_acc[...] = sq_acc[...] + weight * (both * outer)

    carry[...] = jnp.zeros_like(carry)
    sq_acc[...] = jnp.zeros_like(sq_acc)
    gat[top, diagonals] = jnp.zeros(gat.shape[2:], F32)
    flats[...] = jnp.zeros_like(flats)
    for copy in early:
        copy.wait()
    factors(top, steps - 1)

    def take(layer, d):
        before = d - 1
        if layer == top:
            before = d - 1 if isinstance(d, int) else jnp.where(d == 0, diagonals, d - 1)
            when(d > 0, functools.partial(finish_c, layer, d - 1))
        else:
            finish_c(layer, d - 1)
        cell(layer, before, step_of(layer, d))

    def spread(layer, d):
        step = step_of(layer, d)
        if layer == top:
            send_product(rec_w, layer, step, layer, d, False)
            return

        def alone():
            for dh in range(1, ratio):
                start_a(layer, d, dh)

        when(step < steps, functools.partial(send_product, rec_w, layer, step, layer, d, True))
        when(step >= steps, alone)

    def ready(which, weights, layer):
        load(which, layer).wait()
        unfold(which, weights, layer)
        if layer > 0:
            load(which, layer - 1).start()

    def when(condition, step):
        if isinstance(condition, bool):
            if condition:
                step()
        else:
            pl.when(condition)(step)

    def both(first, second):
        return first and second if isinstance(first, bool) else first & second

    def running(d):
        return both(d >= top, d <= diagonals - 1)

    def opening(d):
        for layer in range(top, -1, -1):
            when(active(layer, d), functools.partial(take, layer, d))
            if layer == top:
                when(d == 0, functools.partial(ready, 0, rec_w, layer))
            when(feeds(layer, d), functools.partial(spread, layer, d))
            if layer == top:
                when(running(d - 1), functools.partial(finish_r, kind_in, d - 1))
            if layer > 0:
                def pass_down(layer=layer):
                    when(d == top - layer, functools.partial(ready, 1, in_w, layer))
                    for dh in range(ratio):
                        product(in_w, layer, step_of(layer, d), layer - 1, d, dh, False)

                when(feeds(layer - 1, d), pass_down)

        def bottom():
            when(d == top, functools.partial(ready, 1, in_w, 0))
            send_product(in_w, 0, step_of(0, d), kind_in, d, False)

        when(running(d), bottom)

    def fill_gram(layer, d):
        when(active(layer, d), functools.partial(grams, layer, step_of(layer, d)))

    def fill_factors(layer, d):
        when(active(layer, d + 1), functools.partial(factors, layer, step_of(layer, d + 1)))

    def diagonal(d, _):
        opening(d)
        for layer in range(top, -1, -1):
            when(feeds(layer, d), functools.partial(finish_a, layer, d))
            if layer == top:
                @pl.when(d == 0)
                def _():
                    for copy in rest:
                        copy.wait()

                fill_gram(layer, d)
            else:
                when(running(d - 1), functools.partial(finish_b, kind_in, d - 1))
                fill_factors(layer + 1, d)
            when(feeds(layer, d), functools.partial(finish_r, layer, d))
            if layer < top:
                when(d == top - layer - 1, functools.partial(ready, 0, rec_w, layer))
                fill_gram(layer, d)
        for layer in range(top, -1, -1):
            when(feeds(layer, d), functools.partial(finish_b, layer, d))
            if layer == top:
                when(running(d), functools.partial(finish_a, kind_in, d))
            if layer > 0:
                fill_factors(layer - 1, d)
        return 0

    def sq_copy_a(offset):
        slot = slot_of[offset]
        return remote(sq_mine, sq_a.at[slot], qsa.at[slot], qra.at[slot], plane_peer(*offset))

    def sq_copy_b(dz):
        return remote(sq_sum, sq_b.at[dz - 1], qsb.at[dz - 1], qrb.at[dz - 1], line_peer(dz))

    def collect(d):
        finish_c(kind_in, d)
        input_grad[step_of(0, d)] = gat[kind_in, d]

    def settle(d, _):
        for layer in range(layers):
            pl.when(feeds(layer, d))(functools.partial(sent, layer, d))
        return 0

    def settle_in(d, _):
        sent(kind_in, d)
        return 0

    final = diagonals - 1
    lax.fori_loop(0, final, diagonal, 0)
    opening(final)
    fill_gram(0, final)
    sq_mine[...] = jnp.full(sq_mine.shape, jnp.sum(sq_acc[...]), F32)
    for offset in plane:
        sq_copy_a(offset).start()
    finish_a(kind_in, final)
    value = sq_mine[...]
    for offset in plane:
        sq_copy_a(offset).wait_recv()
        value = value + sq_a[slot_of[offset]]
    sq_sum[...] = value
    for dz in range(1, rows):
        sq_copy_b(dz).start()
    finish_b(kind_in, final - 1)
    finish_r(kind_in, final)
    lax.fori_loop(0, diagonals, settle, 0)

    def gather(d, _):
        collect(d)
        return 0

    lax.fori_loop(top, final, gather, 0)
    value = sq_sum[...]
    for dz in range(1, rows):
        sq_copy_b(dz).wait_recv()
        value = value + sq_b[dz - 1]
    squares[...] = value
    for offset in plane:
        sq_copy_a(offset).wait_send()
    for dz in range(1, rows):
        sq_copy_b(dz).wait_send()
    finish_b(kind_in, final)
    lax.fori_loop(top, final, settle_in, 0)
    collect(final)
    sent(kind_in, final)


def recurrence(w_rec, w_in, gate_pre, cells, top_grad, h_prev, layer_in):
    rows, cols = lax.axis_size("row"), lax.axis_size("col")
    ratio = cols // rows
    layers, row_units, _, units = w_rec.shape
    steps, batch, _ = top_grad.shape
    diagonals = steps + layers - 1
    piece = batch // rows
    cores = 2 if rows % 2 == 0 else 1
    lots = rows // cores
    kinds = layers + 1
    group = rows * ratio - 1
    dma = pltpu.SemaphoreType.DMA
    vmem = lambda *shape: pltpu.VMEM(shape, F32)
    in_vmem = pl.BlockSpec(memory_space=pltpu.VMEM)
    in_any = pl.BlockSpec(memory_space=pl.ANY)
    return pl.pallas_call(
        functools.partial(recurrence_kernel, rows, cores, ratio, layers, steps),
        out_shape=[
            jax.ShapeDtypeStruct((layers, steps * batch, 4 * units), BF16),
            jax.ShapeDtypeStruct((steps, batch, units), F32),
            jax.ShapeDtypeStruct((8, 128), F32),
        ],
        in_specs=[in_any] * 7,
        out_specs=[in_vmem] * 3,
        scratch_shapes=[
            pltpu.VMEM((layers, 4, units, row_units), BF16), pltpu.VMEM((layers, 4, units, row_units), BF16),
            pltpu.VMEM((2, row_units, 4, units), BF16), vmem(units // 128, 4 * 128, 128),
            vmem(*gate_pre.shape), vmem(*cells.shape), vmem(*top_grad.shape),
            pltpu.VMEM(h_prev.shape, BF16), pltpu.VMEM(layer_in.shape, BF16),
            vmem(layers, 6, batch, units), vmem(layers, batch, units), vmem(batch, steps * batch),
            vmem(kinds, diagonals, batch, row_units), vmem(kinds, diagonals, ratio - 1, lots, cores, piece, units),
            vmem(kinds, diagonals, lots, cores, piece, units), vmem(kinds, diagonals, max(lots - 1, 1), cores, piece, units),
            vmem(kinds, diagonals, rows, piece, units),
            vmem(kinds, diagonals + 1, batch, units),
            vmem(8, 128), vmem(group, 8, 128), vmem(8, 128), vmem(rows - 1, 8, 128),
            dma((2,)), dma((4 + 2 * layers,)),
            dma((kinds, diagonals, ratio - 1, lots, cores)), dma((kinds, diagonals, ratio - 1, lots, cores)),
            dma((kinds, diagonals, max(lots - 1, 1), cores)), dma((kinds, diagonals, max(lots - 1, 1), cores)),
            dma((kinds, diagonals, lots, cores)), dma((kinds, diagonals, rows)),
            dma((kinds, diagonals, rows - 1)), dma((kinds, diagonals, rows - 1)),
            dma((group,)), dma((group,)), dma((rows - 1,)), dma((rows - 1,)),
        ],
        compiler_params=pltpu.CompilerParams(collective_id=0, has_side_effects=True, vmem_limit_bytes=VMEM_BYTES),
        name="recurrence",
    )(w_rec, w_in, gate_pre, cells, top_grad, h_prev, layer_in)


def weight_kernel(entries, squares, h_prev, layer_in, flats, rec_out, in_out, stage):
    scale = 1.0 / jnp.maximum(jnp.sqrt(squares[...] / entries), 0.05)
    tall, units = rec_out.shape[1], rec_out.shape[3]
    scale = jnp.broadcast_to(scale[:1, :1], (tall, units))
    for source, out in ((h_prev, rec_out), (layer_in, in_out)):
        left = source[0].T
        for gate in range(4):
            value = contract(left, flats[0, :, gate * units:(gate + 1) * units], ((1,), (0,))) * scale
            for lane in range(units // 128):
                stage[lane, pl.ds(gate, tall, stride=4), :] = value[:, lane * 128:(lane + 1) * 128]
        for lane in range(units // 128):
            out[0, :, :, lane * 128:(lane + 1) * 128] = stage[lane].reshape(tall, 4, 128).astype(BF16)


def weight_grads(squares, h_prev, layer_in, flats, entries):
    layers, tokens, row_units = h_prev.shape
    units = flats.shape[2] // 4
    tall = tile_of(row_units, 512)
    source = pl.BlockSpec((1, tokens, tall), lambda layer, tile: (layer, 0, tile))
    target = pl.BlockSpec((1, tall, 4, units), lambda layer, tile: (layer, tile, 0, 0))
    shape = jax.ShapeDtypeStruct((layers, row_units, 4, units), BF16)
    return pl.pallas_call(
        functools.partial(weight_kernel, entries),
        grid=(layers, row_units // tall),
        out_shape=[shape, shape],
        in_specs=[
            pl.BlockSpec((8, 128), lambda layer, tile: (0, 0)),
            source, source,
            pl.BlockSpec((1, tokens, 4 * units), lambda layer, tile: (layer, 0, 0)),
        ],
        out_specs=[target, target],
        scratch_shapes=[pltpu.VMEM((units // 128, 4 * tall, 128), F32)],
        compiler_params=pltpu.CompilerParams(vmem_limit_bytes=VMEM_BYTES),
        name="weight_grads",
    )(squares, h_prev, layer_in, flats)


def local(w_rec, w_in, gate_pre, cells, layer_in, h_prev, top_grad):
    layers, row_units = w_rec.shape[:2]
    steps, batch, units = top_grad.shape
    rec_in = h_prev.reshape(layers, steps * batch, row_units)
    lay_in = layer_in.reshape(layers, steps * batch, row_units)
    flats, input_grad, squares = recurrence(w_rec, w_in, gate_pre, cells, top_grad, rec_in, lay_in)
    entries = 2.0 * layers * (row_units * lax.axis_size("row")) * (4 * units * lax.axis_size("col"))
    rec_grad, in_grad = weight_grads(squares, rec_in, lay_in, flats, entries)
    return (rec_grad, in_grad, input_grad)


def solution(mesh):
    placed = (
        P(None, "row", None, "col"),
        P(None, "row", None, "col"),
        P(None, None, None, None, "col"),
        P(None, None, None, "col"),
        P(None, None, None, "row"),
        P(None, None, None, "row"),
        P(None, None, "col"),
    )
    return jax.shard_map(
        local,
        mesh=mesh,
        in_specs=placed,
        out_specs=(P(None, "row", None, "col"), P(None, "row", None, "col"), P(None, None, "col")),
        check_vma=False,
    )
```

```python
import functools

import jax
import jax.numpy as jnp
from jax import lax
from jax.experimental import pallas as pl
from jax.experimental.pallas import tpu as pltpu
from jax.sharding import PartitionSpec as P

MESH = pl.DeviceIdType.MESH
F32 = jnp.float32
BF16 = jnp.bfloat16
VMEM_BYTES = 63 * 1024 * 1024


def contract(left, right, dims):
    return lax.dot_general(left, right, ((dims[0], dims[1]), ((), ())), preferred_element_type=F32)


def tile_of(size, limit):
    while size % limit:
        limit //= 2
    return limit


def recurrence_kernel(
    rows, cores, ratio, layers, steps,
    w_rec, w_in, gate_pre_any, cells_any, top_grad_any, h_prev_any, layer_in_any,
    flats, input_grad, squares,
    rec_w, in_w, raw, fold, gate_pre, cells, top_grad, h_prev, layer_in, fac, carry, sq_acc, part, recv_a, acc, recv_r, recv_b, gat, sq_mine, sq_a, sq_sum, sq_b,
    w_sem, e_sem, sa, ra, sr, rr, sb, rb, sc, rc, qsa, qra, qsb, qrb,
):
    top = layers - 1
    diagonals = steps + top
    batch, units = top_grad_any.shape[1:]
    piece = batch // rows
    kind_in = layers
    row = lax.axis_index("row")
    col = lax.axis_index("col")
    deep, half = col // ratio, col % ratio
    lots = rows // cores
    lot, core = row // cores, row % cores
    inside = core == deep % cores

    def load(which, layer):
        return pltpu.make_async_copy((w_rec, w_in)[which].at[layer], raw.at[which], w_sem.at[which])

    def move(src, dst, at, index):
        return pltpu.make_async_copy(src.at[at], dst.at[at], e_sem.at[index])

    late = steps - 1
    early = [
        move(gate_pre_any, gate_pre, (top, late), 0),
        move(cells_any, cells, top, 1),
        move(top_grad_any, top_grad, slice(None), 2),
    ]
    rest = [move(gate_pre_any, gate_pre, (top, slice(0, late)), 3)] if late else []
    for layer in range(top):
        rest.append(move(gate_pre_any, gate_pre, layer, 4 + 2 * layer))
        rest.append(move(cells_any, cells, layer, 5 + 2 * layer))
    rest.append(move(h_prev_any, h_prev, slice(None), 4 + 2 * top))
    rest.append(move(layer_in_any, layer_in, slice(None), 5 + 2 * top))
    for copy in early:
        copy.start()
    for which in range(2):
        load(which, top).start()
    for copy in rest:
        copy.start()

    plane = [(dr, dh) for dr in range(rows) for dh in range(ratio)][1:]
    slot_of = {offset: index for index, offset in enumerate(plane)}

    def plane_peer(dr, dh):
        return ((row + dr) % rows, deep * ratio + (half + dh) % ratio)

    def line_peer(dz):
        return (row, ((deep + dz) % rows) * ratio + half)

    def row_peer(dq):
        return ((row + dq) % rows, col)

    barrier = pltpu.get_barrier_semaphore()
    for offset in plane:
        pl.semaphore_signal(barrier, inc=1, device_id=plane_peer(*offset), device_id_type=MESH)
    for dz in range(1, rows):
        pl.semaphore_signal(barrier, inc=1, device_id=line_peer(dz), device_id_type=MESH)
    for dz in range(rows):
        source = (lot * cores + deep % cores, ((deep - dz + rows) % rows) * ratio + half)
        if dz:
            pl.semaphore_signal(barrier, inc=1, device_id=source, device_id_type=MESH)
        else:
            @pl.when(jnp.logical_not(inside))
            def _(source=source):
                pl.semaphore_signal(barrier, inc=1, device_id=source, device_id_type=MESH)


    def remote(src, dst, send, recv, device):
        return pltpu.make_async_remote_copy(
            src_ref=src, dst_ref=dst, send_sem=send, recv_sem=recv, device_id=device, device_id_type=MESH
        )

    def quarter(index):
        return pl.ds(pl.multiple_of(index * piece, piece), piece)

    def lanes(index, size):
        return pl.ds(pl.multiple_of(index * size, size), size)

    turns = [(dx, dg) for dx in list(range(1, lots)) + [0] for dg in list(range(1, cores)) + [0]]

    def block_of(dx, dg):
        return ((lot + dx) % lots) * cores + (core + dg) % cores

    def copy_a(kind, d, dh, dx, dg):
        src = part.at[kind, d, quarter(block_of(dx, dg)), lanes((half + dh) % ratio, units)]
        spot = (kind, d, dh - 1, dx, dg)
        return remote(src, recv_a.at[spot], sa.at[spot], ra.at[spot], plane_peer(0, dh))

    def copy_r(kind, d, dx, dg):
        spot = (kind, d, dx - 1, dg)
        return remote(acc.at[kind, d, dx, dg], recv_r.at[spot], sr.at[spot], rr.at[spot], (block_of(dx, 0), col))

    def origin(dx):
        return block_of(lots - dx, 0)

    def copy_b(kind, d, dx, dg):
        src = recv_r.at[kind, d, dx - 1, dg] if dx else acc.at[kind, d, 0, dg]
        slot = (origin(dx) - deep + rows) % rows
        peer = (block_of(0, dg), origin(dx) * ratio + half)
        return remote(src, recv_b.at[kind, d, slot], sb.at[kind, d, dx, dg], rb.at[kind, d, slot], peer)

    def copy_c(kind, d, dq):
        spot = gat.at[kind, d, quarter(row)]
        return remote(spot, spot, sc.at[kind, d, dq - 1], rc.at[kind, d, dq - 1], row_peer(dq))

    def start_a(kind, d, dh):
        for dx, dg in turns:
            copy_a(kind, d, dh, dx, dg).start()

    def finish_a(kind, d):
        for dx, dg in turns:
            value = part[kind, d, quarter(block_of(dx, dg)), lanes(half, units)]
            for dh in range(1, ratio):
                copy_a(kind, d, dh, dx, dg).wait_recv()
                value = value + recv_a[kind, d, dh - 1, dx, dg]
            if dx:
                acc[kind, d, dx, dg] = value
                copy_r(kind, d, dx, dg).start()
            elif dg:
                acc[kind, d, 0, dg] = value
                copy_b(kind, d, 0, dg).start()
            else:
                home = row == deep

                @pl.when(home)
                def _():
                    recv_b[kind, d, 0] = value

                @pl.when(jnp.logical_not(home))
                def _():
                    acc[kind, d, 0, 0] = value
                    copy_b(kind, d, 0, 0).start()

    def finish_r(kind, d):
        for dx in range(1, lots):
            for dg in list(range(1, cores)) + [0]:
                copy_r(kind, d, dx, dg).wait_recv()
                if dg:
                    copy_b(kind, d, dx, dg).start()
                else:
                    home = origin(dx) == deep

                    @pl.when(home)
                    def _():
                        recv_b[kind, d, 0] = recv_r[kind, d, dx - 1, 0]

                    @pl.when(jnp.logical_not(home))
                    def _():
                        copy_b(kind, d, dx, 0).start()

    def source_of(dz):
        return (lot * cores + deep % cores, ((deep - dz + rows) % rows) * ratio + half)

    def arrival(kind, d, dz):
        return remote(acc.at[kind, d, 0, 0], recv_b.at[kind, d, dz], sb.at[kind, d, 0, 0], rb.at[kind, d, dz], source_of(dz))

    def finish_b(kind, d):
        @pl.when(jnp.logical_not(inside))
        def _():
            arrival(kind, d, 0).wait_recv()

        for dz in range(1, rows):
            arrival(kind, d, dz).wait_recv()
        value = recv_b[kind, d, 0]
        for dz in range(1, rows):
            value = value + recv_b[kind, d, dz]
        gat[kind, d, quarter(row)] = value
        for dq in range(1, rows):
            copy_c(kind, d, dq).start()

    def finish_c(kind, d):
        for dq in range(1, rows):
            spot = gat.at[kind, d, quarter((row - dq + rows) % rows)]
            remote(spot, spot, sc.at[kind, d, dq - 1], rc.at[kind, d, dq - 1], row_peer(dq)).wait_recv()

    def sent(kind, d):
        for dx, dg in turns:
            for dh in range(1, ratio):
                copy_a(kind, d, dh, dx, dg).wait_send()
            if dx:
                copy_r(kind, d, dx, dg).wait_send()
            if dg:
                copy_b(kind, d, dx, dg).wait_send()
            else:
                @pl.when(origin(dx) != deep)
                def _(dx=dx):
                    copy_b(kind, d, dx, 0).wait_send()

        for dq in range(1, rows):
            copy_c(kind, d, dq).wait_send()

    def step_of(layer, d):
        return steps - 1 - d + top - layer

    def active(layer, d):
        return both(d >= top - layer, d <= top - layer + steps - 1)

    def feeds(layer, d):
        first = top - layer - 1 if layer < top else 0
        return both(d >= first, d <= top - layer + steps - 2)

    chunk = 16

    def factors(layer, step):
        def body(index, _):
            at = pl.ds(pl.multiple_of(index * chunk, chunk), chunk)
            in_gate = jax.nn.sigmoid(gate_pre[layer, step, at, 0, :])
            forget = jax.nn.sigmoid(gate_pre[layer, step, at, 1, :])
            cand = jnp.tanh(gate_pre[layer, step, at, 2, :])
            out_gate = jax.nn.sigmoid(gate_pre[layer, step, at, 3, :])
            tanh_cell = jnp.tanh(cells[layer, step + 1, at, :])
            fac[layer, 0, at, :] = out_gate * (1.0 - tanh_cell * tanh_cell)
            fac[layer, 1, at, :] = cand * in_gate * (1.0 - in_gate)
            fac[layer, 2, at, :] = cells[layer, step, at, :] * forget * (1.0 - forget)
            fac[layer, 3, at, :] = in_gate * (1.0 - cand * cand)
            fac[layer, 4, at, :] = tanh_cell * out_gate * (1.0 - out_gate)
            fac[layer, 5, at, :] = forget
            return 0

        lax.fori_loop(0, batch // chunk, body, 0)

    def cell(layer, d, step):
        def body(index, _):
            at = pl.ds(pl.multiple_of(index * chunk, chunk), chunk)
            out_at = pl.ds(pl.multiple_of(step * batch + index * chunk, chunk), chunk)
            if layer == top:
                hid = top_grad[step, at, :] + gat[layer, d, at, :]
            else:
                hid = gat[layer, d, at, :]
            grad = carry[layer, at, :] + hid * fac[layer, 0, at, :]
            for gate in range(3):
                flats[layer, out_at, gate * units:(gate + 1) * units] = (grad * fac[layer, gate + 1, at, :]).astype(BF16)
            flats[layer, out_at, 3 * units:] = (hid * fac[layer, 4, at, :]).astype(BF16)
            carry[layer, at, :] = grad * fac[layer, 5, at, :]
            return 0

        lax.fori_loop(0, batch // chunk, body, 0)

    row_units = part.shape[-1]

    def rows_of(step):
        return pl.ds(step * batch if isinstance(step, int) else pl.multiple_of(step * batch, batch), batch)

    def product(weights, layer, step, kind, d, dh, add):
        at = rows_of(step)
        spot = lanes((half + dh) % ratio, units)
        value = part[kind, d, :, spot] if add else None
        for gate in range(4):
            new = contract(flats[layer, at, gate * units:(gate + 1) * units], weights[layer, gate, :, spot], ((1,), (0,)))
            value = new if value is None else value + new
        part[kind, d, :, spot] = value

    def send_product(weights, layer, step, kind, d, add):
        for dh in list(range(1, ratio)) + [0]:
            product(weights, layer, step, kind, d, dh, add)
            if dh:
                start_a(kind, d, dh)

    tall = 128

    def unfold(which, weights, layer):
        def body(index, _):
            at = pl.ds(pl.multiple_of(index * tall, tall), tall)
            for lane in range(units // 128):
                span = slice(lane * 128, (lane + 1) * 128)
                fold[lane] = raw[which, at, :, span].astype(F32).reshape(4 * tall, 128)
            for lane in range(units // 128):
                span = slice(lane * 128, (lane + 1) * 128)
                for gate in range(4):
                    weights[layer, gate, span, at] = fold[lane, pl.ds(gate, tall, stride=4), :].astype(BF16).T
            return 0

        lax.fori_loop(0, row_units // tall, body, 0)


    def grams(layer):
        outer = contract(h_prev[layer], h_prev[layer], ((1,), (1,))) + contract(layer_in[layer], layer_in[layer], ((1,), (1,)))
        whole = contract(flats[layer], flats[layer], ((1,), (1,)))
        sq_acc[...] = sq_acc[...] + outer * whole

    carry[...] = jnp.zeros_like(carry)
    sq_acc[...] = jnp.zeros_like(sq_acc)
    gat[top, diagonals] = jnp.zeros(gat.shape[2:], F32)
    for copy in early:
        copy.wait()
    factors(top, steps - 1)

    def take(layer, d):
        before = d - 1
        if layer == top:
            before = d - 1 if isinstance(d, int) else jnp.where(d == 0, diagonals, d - 1)
            when(d > 0, functools.partial(finish_c, layer, d - 1))
        else:
            finish_c(layer, d - 1)
        cell(layer, before, step_of(layer, d))

    def spread(layer, d):
        step = step_of(layer, d)
        if layer == top:
            send_product(rec_w, layer, step, layer, d, False)
            return

        def alone():
            for dh in range(1, ratio):
                start_a(layer, d, dh)

        when(step < steps, functools.partial(send_product, rec_w, layer, step, layer, d, True))
        when(step >= steps, alone)

    def ready(which, weights, layer):
        load(which, layer).wait()
        unfold(which, weights, layer)
        if layer > 0:
            load(which, layer - 1).start()

    def when(condition, step):
        if isinstance(condition, bool):
            if condition:
                step()
        else:
            pl.when(condition)(step)

    def both(first, second):
        return first and second if isinstance(first, bool) else first & second

    def running(d):
        return both(d >= top, d <= diagonals - 1)

    def opening(d):
        for layer in range(top, -1, -1):
            when(active(layer, d), functools.partial(take, layer, d))
            when(feeds(layer, d), functools.partial(spread, layer, d))
            if layer == top:
                when(running(d - 1), functools.partial(finish_r, kind_in, d - 1))
            if layer > 0:
                def pass_down(layer=layer):
                    when(d == top - layer, functools.partial(ready, 1, in_w, layer))
                    for dh in range(ratio):
                        product(in_w, layer, step_of(layer, d), layer - 1, d, dh, False)

                when(feeds(layer - 1, d), pass_down)

        def bottom():
            when(d == top, functools.partial(ready, 1, in_w, 0))
            send_product(in_w, 0, step_of(0, d), kind_in, d, False)

        return bottom

    def fill_gram(layer, d):
        when(d == top - layer + steps - 1, functools.partial(grams, layer))

    def fill_factors(layer, d):
        when(active(layer, d + 1), functools.partial(factors, layer, step_of(layer, d + 1)))

    def diagonal(d, _):
        bottom = opening(d)
        for layer in range(top, -1, -1):
            when(feeds(layer, d), functools.partial(finish_a, layer, d))
            if layer == top:
                when(running(d), bottom)

                @pl.when(d == 0)
                def _():
                    for copy in rest:
                        copy.wait()

                fill_gram(layer, d)
            else:
                when(running(d - 1), functools.partial(finish_b, kind_in, d - 1))
                fill_factors(layer + 1, d)
            when(feeds(layer, d), functools.partial(finish_r, layer, d))
            if layer < top:
                when(d == top - layer - 1, functools.partial(ready, 0, rec_w, layer))
                fill_gram(layer, d)
        for layer in range(top, -1, -1):
            when(feeds(layer, d), functools.partial(finish_b, layer, d))
            if layer == top:
                when(running(d), functools.partial(finish_a, kind_in, d))
            if layer > 0:
                fill_factors(layer - 1, d)
        return 0

    def sq_copy_a(offset):
        slot = slot_of[offset]
        return remote(sq_mine, sq_a.at[slot], qsa.at[slot], qra.at[slot], plane_peer(*offset))

    def sq_copy_b(dz):
        return remote(sq_sum, sq_b.at[dz - 1], qsb.at[dz - 1], qrb.at[dz - 1], line_peer(dz))

    def collect(d):
        finish_c(kind_in, d)
        input_grad[step_of(0, d)] = gat[kind_in, d]

    def settle(d, _):
        for layer in range(layers):
            pl.when(feeds(layer, d))(functools.partial(sent, layer, d))
        return 0

    def settle_in(d, _):
        sent(kind_in, d)
        return 0

    final = diagonals - 1
    ready(0, rec_w, top)
    pl.semaphore_wait(barrier, len(plane) + rows - 1 + rows - jnp.where(inside, 1, 0))
    lax.fori_loop(0, final, diagonal, 0)
    opening(final)()
    fill_gram(0, final)
    sq_mine[...] = jnp.full(sq_mine.shape, jnp.sum(sq_acc[...]), F32)
    for offset in plane:
        sq_copy_a(offset).start()
    finish_a(kind_in, final)
    value = sq_mine[...]
    for offset in plane:
        sq_copy_a(offset).wait_recv()
        value = value + sq_a[slot_of[offset]]
    sq_sum[...] = value
    for dz in range(1, rows):
        sq_copy_b(dz).start()
    finish_b(kind_in, final - 1)
    finish_r(kind_in, final)
    lax.fori_loop(0, diagonals, settle, 0)

    def gather(d, _):
        collect(d)
        return 0

    lax.fori_loop(top, final, gather, 0)
    value = sq_sum[...]
    for dz in range(1, rows):
        sq_copy_b(dz).wait_recv()
        value = value + sq_b[dz - 1]
    squares[...] = value
    for offset in plane:
        sq_copy_a(offset).wait_send()
    for dz in range(1, rows):
        sq_copy_b(dz).wait_send()
    finish_b(kind_in, final)
    lax.fori_loop(top, final, settle_in, 0)
    collect(final)
    sent(kind_in, final)


def recurrence(w_rec, w_in, gate_pre, cells, top_grad, h_prev, layer_in):
    rows, cols = lax.axis_size("row"), lax.axis_size("col")
    ratio = cols // rows
    layers, row_units, _, units = w_rec.shape
    steps, batch, _ = top_grad.shape
    diagonals = steps + layers - 1
    piece = batch // rows
    cores = 2 if rows % 2 == 0 else 1
    lots = rows // cores
    kinds = layers + 1
    group = rows * ratio - 1
    dma = pltpu.SemaphoreType.DMA
    vmem = lambda *shape: pltpu.VMEM(shape, F32)
    in_vmem = pl.BlockSpec(memory_space=pltpu.VMEM)
    in_any = pl.BlockSpec(memory_space=pl.ANY)
    return pl.pallas_call(
        functools.partial(recurrence_kernel, rows, cores, ratio, layers, steps),
        out_shape=[
            jax.ShapeDtypeStruct((layers, steps * batch, 4 * units), BF16),
            jax.ShapeDtypeStruct((steps, batch, units), F32),
            jax.ShapeDtypeStruct((8, 128), F32),
        ],
        in_specs=[in_any] * 7,
        out_specs=[in_vmem] * 3,
        scratch_shapes=[
            pltpu.VMEM((layers, 4, units, row_units), BF16), pltpu.VMEM((layers, 4, units, row_units), BF16),
            pltpu.VMEM((2, row_units, 4, units), BF16), vmem(units // 128, 4 * 128, 128),
            vmem(*gate_pre.shape), vmem(*cells.shape), vmem(*top_grad.shape),
            pltpu.VMEM(h_prev.shape, BF16), pltpu.VMEM(layer_in.shape, BF16),
            vmem(layers, 6, batch, units), vmem(layers, batch, units), vmem(steps * batch, steps * batch),
            vmem(kinds, diagonals, batch, row_units), vmem(kinds, diagonals, ratio - 1, lots, cores, piece, units),
            vmem(kinds, diagonals, lots, cores, piece, units), vmem(kinds, diagonals, max(lots - 1, 1), cores, piece, units),
            vmem(kinds, diagonals, rows, piece, units),
            vmem(kinds, diagonals + 1, batch, units),
            vmem(8, 128), vmem(group, 8, 128), vmem(8, 128), vmem(rows - 1, 8, 128),
            dma((2,)), dma((4 + 2 * layers,)),
            dma((kinds, diagonals, ratio - 1, lots, cores)), dma((kinds, diagonals, ratio - 1, lots, cores)),
            dma((kinds, diagonals, max(lots - 1, 1), cores)), dma((kinds, diagonals, max(lots - 1, 1), cores)),
            dma((kinds, diagonals, lots, cores)), dma((kinds, diagonals, rows)),
            dma((kinds, diagonals, rows - 1)), dma((kinds, diagonals, rows - 1)),
            dma((group,)), dma((group,)), dma((rows - 1,)), dma((rows - 1,)),
        ],
        compiler_params=pltpu.CompilerParams(collective_id=0, has_side_effects=True, vmem_limit_bytes=VMEM_BYTES),
        name="recurrence",
    )(w_rec, w_in, gate_pre, cells, top_grad, h_prev, layer_in)


def weight_kernel(entries, squares, h_prev, layer_in, flats, rec_out, in_out, stage):
    scale = 1.0 / jnp.maximum(jnp.sqrt(squares[...] / entries), 0.05)
    tall, units = rec_out.shape[1], rec_out.shape[3]
    wide = tile_of(units, 256)
    scale = jnp.broadcast_to(scale[:1, :1], (2 * tall, wide))
    left = jnp.concatenate([h_prev[0].T, layer_in[0].T], axis=0)
    for tile in range(units // wide):
        for gate in range(4):
            start = gate * units + tile * wide
            value = contract(left, flats[0, :, start:start + wide], ((1,), (0,))) * scale
            for lane in range(wide // 128):
                stage[lane, pl.ds(gate, 2 * tall, stride=4), :] = value[:, lane * 128:(lane + 1) * 128]
        for lane in range(wide // 128):
            span = slice(tile * wide + lane * 128, tile * wide + (lane + 1) * 128)
            rec_out[0, :, :, span] = stage[lane, :4 * tall].reshape(tall, 4, 128).astype(BF16)
            in_out[0, :, :, span] = stage[lane, 4 * tall:].reshape(tall, 4, 128).astype(BF16)


def weight_grads(squares, h_prev, layer_in, flats, entries):
    layers, tokens, row_units = h_prev.shape
    units = flats.shape[2] // 4
    tall = tile_of(row_units, 512)
    source = pl.BlockSpec((1, tokens, tall), lambda layer, tile: (layer, 0, tile))
    target = pl.BlockSpec((1, tall, 4, units), lambda layer, tile: (layer, tile, 0, 0))
    shape = jax.ShapeDtypeStruct((layers, row_units, 4, units), BF16)
    return pl.pallas_call(
        functools.partial(weight_kernel, entries),
        grid=(layers, row_units // tall),
        out_shape=[shape, shape],
        in_specs=[
            pl.BlockSpec((8, 128), lambda layer, tile: (0, 0)),
            source, source,
            pl.BlockSpec((1, tokens, 4 * units), lambda layer, tile: (layer, 0, 0)),
        ],
        out_specs=[target, target],
        scratch_shapes=[pltpu.VMEM((tile_of(units, 256) // 128, 8 * tall, 128), F32)],
        compiler_params=pltpu.CompilerParams(vmem_limit_bytes=VMEM_BYTES),
        name="weight_grads",
    )(squares, h_prev, layer_in, flats)


def local(w_rec, w_in, gate_pre, cells, layer_in, h_prev, top_grad):
    layers, row_units = w_rec.shape[:2]
    steps, batch, units = top_grad.shape
    rec_in = h_prev.reshape(layers, steps * batch, row_units)
    lay_in = layer_in.reshape(layers, steps * batch, row_units)
    flats, input_grad, squares = recurrence(w_rec, w_in, gate_pre, cells, top_grad, rec_in, lay_in)
    entries = 2.0 * layers * (row_units * lax.axis_size("row")) * (4 * units * lax.axis_size("col"))
    rec_grad, in_grad = weight_grads(squares, rec_in, lay_in, flats, entries)
    return (rec_grad, in_grad, input_grad)


def solution(mesh):
    placed = (
        P(None, "row", None, "col"),
        P(None, "row", None, "col"),
        P(None, None, None, None, "col"),
        P(None, None, None, "col"),
        P(None, None, None, "row"),
        P(None, None, None, "row"),
        P(None, None, "col"),
    )
    return jax.shard_map(
        local,
        mesh=mesh,
        in_specs=placed,
        out_specs=(P(None, "row", None, "col"), P(None, "row", None, "col"), P(None, None, "col")),
        check_vma=False,
    )
```
